128 devices in a mesh: rows: 64 (over x, y, z_lo, core), res: 2 (over z_hi).
Axes of the slice: x: 4, y: 4, z: 4 (z_hi: 2, z_lo: 2; z = z_hi * 2 + z_lo), core: 2. Of those that a mesh axis runs over, the one named last changes fastest.
Arguments:
- base_runs: bfloat16 [262144, 32], P(('rows', 'res')), may hold values from -100 to 100
- other_runs: bfloat16 [262144, 32], P(('rows', 'res')), may hold values from -100 to 100
- mixed_runs: bfloat16 [262144, 4096], P(('rows', 'res')), may hold values from -100 to 100
- counts: int32 [256, 262144], P(None, ('rows', 'res')), may hold values from 0 to 4
Outputs:
- first_order: float32 [256, 4096], P('res', 'rows')
- total_order: float32 [256, 4096], P('res', 'rows')
The draws below stay inside these ranges and needn't reach their ends.
All inputs are finite; a program needn't handle non-finite values.
Results may differ from the reference program's by a relative error of at most 0.0003.
Values sent between devices are 32-bit elements; how exact they have to be, the bound alone decides.
A program may use at most 192 MiB of HBM per device.

```python
import jax
import jax.numpy as jnp
from jax import lax

D = 128
M = 32
K = 256
ROW_DEV = 2048
SAMPLES = 262144


def runs_joint(key):
    streams = jax.random.split(jax.random.fold_in(key, 7), 6)
    row_scale = 10.0 ** jax.random.uniform(streams[0], (SAMPLES, 1), jnp.float32, 0.0, 1.0)
    base_noise = jnp.clip(jax.random.normal(streams[1], (SAMPLES, M), jnp.float32), -5.0, 5.0)
    other_noise = jnp.clip(jax.random.normal(streams[2], (SAMPLES, M), jnp.float32), -5.0, 5.0)
    return (base_noise * row_scale, other_noise * row_scale, streams)


def draw_base_runs(key, part):
    base_vals, other_vals, streams = runs_joint(key)
    return base_vals.astype(jnp.bfloat16)


def draw_other_runs(key, part):
    base_vals, other_vals, streams = runs_joint(key)
    return other_vals.astype(jnp.bfloat16)


def draw_mixed_runs(key, part):
    base_vals, other_vals, streams = runs_joint(key)
    mixing = jax.random.uniform(streams[3], (D, M), jnp.float32, 0.0, 1.0)
    spread = jnp.clip(jax.random.normal(streams[4], (SAMPLES, D, M), jnp.float32), -5.0, 5.0)
    spread_scale = 10.0 ** jax.random.uniform(streams[5], (SAMPLES, 1, 1), jnp.float32, 0.0, 1.0)
    mixed_vals = (1.0 - mixing) * base_vals[:, None, :] + mixing * other_vals[:, None, :] + 0.5 * spread_scale * spread
    return mixed_vals.reshape(SAMPLES, D * M).astype(jnp.bfloat16)


def set_ends(array, rng, smallest, largest):
    shape = array.shape
    place = [jax.random.randint(jax.random.fold_in(rng, axis), (), 0, shape[axis]) for axis in range(len(shape))]
    array = array.at[tuple(place)].set(smallest)
    longest = shape.index(max(shape))
    place[longest] = (place[longest] + 1) % shape[longest]
    return array.at[tuple(place)].set(largest)


def setup_inputs(seed: int = 0) -> dict:
    streams_of = jax.random.split(jax.random.key(seed), 5)
    base_runs = draw_base_runs(jax.random.fold_in(streams_of[4], 71), 0)
    other_runs = draw_other_runs(jax.random.fold_in(streams_of[4], 71), 0)
    mixed_runs = draw_mixed_runs(jax.random.fold_in(streams_of[4], 71), 0)
    counts = set_ends(jax.random.randint(streams_of[3], (K, SAMPLES), 0, 5), jax.random.fold_in(streams_of[3], 1), 0, 4).astype(jnp.int32)
    return dict(base_runs=base_runs, other_runs=other_runs, mixed_runs=mixed_runs, counts=counts)


def moment_inputs(base_runs, other_runs, mixed_runs):
    row_total = base_runs.shape[0]
    width = base_runs.shape[1]
    base_wide = base_runs.astype(jnp.float32)
    other_wide = other_runs.astype(jnp.float32)
    mixed_wide = mixed_runs.astype(jnp.float32).reshape(row_total, -1, width)
    change = mixed_wide - base_wide[:, None, :]
    cross = other_wide[:, None, :] * change
    square = change * change
    moment_terms = jnp.concatenate([cross, square], axis=2).reshape(row_total, -1).astype(jnp.bfloat16)
    moments = jnp.concatenate([base_wide + other_wide, base_wide * base_wide + other_wide * other_wide], axis=1).astype(jnp.bfloat16)
    return moment_terms, moments


def indices(weighted, base_sums, total_count, width):
    weight = jnp.maximum(total_count, 1.0)[:, None]
    mean_value = base_sums[:, :width] / (2.0 * weight)
    variance = jnp.maximum(base_sums[:, width:] / (2.0 * weight) - mean_value * mean_value, 0.25)
    shaped = weighted.reshape(weighted.shape[0], -1, 2 * width)
    scaled = (weight * variance)[:, None, :]
    first_order = (shaped[:, :, :width] / scaled).reshape(weighted.shape[0], -1)
    total_order = (shaped[:, :, width:] / (2.0 * scaled)).reshape(weighted.shape[0], -1)
    return first_order, total_order


def reference(base_runs, other_runs, mixed_runs, counts):
    def accumulate(state_tuple, block_index):
        first_row = (block_index * ROW_DEV).astype(jnp.int32)
        base_block = lax.dynamic_slice_in_dim(base_runs, first_row, ROW_DEV, 0)
        other_block = lax.dynamic_slice_in_dim(other_runs, first_row, ROW_DEV, 0)
        mixed_block = lax.dynamic_slice_in_dim(mixed_runs, first_row, ROW_DEV, 0)
        count_block = lax.dynamic_slice_in_dim(counts, first_row, ROW_DEV, 1)
        moment_terms, moments = moment_inputs(base_block, other_block, mixed_block)
        weights = count_block.astype(jnp.bfloat16)
        weighted, base_sums, total_count = state_tuple
        weighted = weighted + jnp.dot(weights, moment_terms, preferred_element_type=jnp.float32)
        base_sums = base_sums + jnp.dot(weights, moments, preferred_element_type=jnp.float32)
        total_count = total_count + jnp.sum(count_block.astype(jnp.float32), axis=1)
        return (weighted, base_sums, total_count), None

    initial = (jnp.zeros((K, 2 * D * M), jnp.float32), jnp.zeros((K, 2 * M), jnp.float32), jnp.zeros((K,), jnp.float32))
    final_state, unused = lax.scan(accumulate, initial, jnp.arange(SAMPLES // ROW_DEV, dtype=jnp.int32))
    first_order, total_order = indices(final_state[0], final_state[1], final_state[2], M)
    return (first_order, total_order)
```

```python
import jax
import jax.numpy as jnp
from jax import lax
from jax.experimental import pallas as pl
from jax.experimental.pallas import tpu as pltpu
from jax.sharding import Mesh
from jax.sharding import PartitionSpec as P

MESH = pl.DeviceIdType.MESH
AXES = ("x", "y", "zl", "core", "zh")

ORDER = (
    (2, 2), (2, 1), (1, 2), (2, 3), (3, 2), (1, 1), (1, 3), (3, 1),
    (3, 3), (2, 0), (0, 2), (1, 0), (0, 1), (3, 0), (0, 3), (0, 0),
)
STEPS = len(ORDER)
DX_CODE = sum(dx << (2 * i) for i, (dx, dy) in enumerate(ORDER))
DY_CODE = sum(dy << (2 * i) for i, (dx, dy) in enumerate(ORDER))
DX_LO, DX_HI = DX_CODE & 0xFFFF, DX_CODE >> 16
DY_LO, DY_HI = DY_CODE & 0xFFFF, DY_CODE >> 16
AHEAD = 6
LAG = 4
ROWS = (((0, 24), (24, 24)), ((48, 24), (72, 16)), ((88, 16), (104, 24)))


def digit(lo, hi, s):
    code = jnp.where(s < 8, lo, hi)
    return lax.shift_right_logical(code, 2 * (s % 8)) & 3


def coords(s):
    s = jnp.asarray(s, jnp.int32)
    return digit(DX_LO, DX_HI, s), digit(DY_LO, DY_HI, s)


def kernel(
    base_hbm, other_hbm, mixed_hbm, counts_hbm,
    first_ref, total_ref,
    base_v, other_v, counts_v, cbf, a4, b4, mbuf, terms0, terms1, stage, part,
    ra0, ra1, rb0, rb1, rc0, rc1,
    q0, q1, q2, q3, q4, q5,
    v0, v1, v2, v3, v4, v5,
    ustage, upart, uz, uy, ux, ufin,
    in_sem, msem, d2d_send, d2d_recv,
    recv1, recv_c, send1, recv2, recv3, send23, usend, urecv,
):
    x = lax.axis_index("x")
    y = lax.axis_index("y")
    zl = lax.axis_index("zl")
    core = lax.axis_index("core")
    zh = lax.axis_index("zh")
    z = zh * 2 + zl

    def at_x(d):
        return {"x": (x + d) % 4}

    def at_y(d):
        return {"y": (y + d) % 4}

    def at_z(d):
        target = (z + d) % 4
        return {"zl": target % 2, "zh": target // 2}

    partner = {"core": 1 - core}
    axes = (at_x, at_y, at_z)

    barrier = pltpu.get_barrier_semaphore()
    peers = [partner] + [ax(d) for ax in axes for d in (1, 2, 3)]
    for peer in peers:
        pl.semaphore_signal(barrier, inc=1, device_id=peer, device_id_type=MESH)

    def mixed_copy(t):
        s = t // 2
        dx, dy = coords(s)
        column = ((((x + dx) % 4) * 4 + (y + dy) % 4) * 2 + (zl + t) % 2) * 128
        return pltpu.make_async_copy(
            mixed_hbm.at[:, pl.ds(pl.multiple_of(column, 128), 128)], mbuf.at[t], msem.at[t]
        )

    counts_copy = pltpu.make_async_copy(counts_hbm, counts_v, in_sem.at[0])
    base_copy = pltpu.make_async_copy(base_hbm, base_v, in_sem.at[1])
    other_copy = pltpu.make_async_copy(other_hbm, other_v, in_sem.at[2])
    base_copy.start()
    other_copy.start()
    counts_copy.start()
    for t in range(AHEAD):
        mixed_copy(t).start()

    lane = lax.broadcasted_iota(jnp.int32, (32, 128), 1)
    row = lax.broadcasted_iota(jnp.int32, (32, 128), 0)
    repeat = (lane % 32 == row).astype(jnp.float32).astype(jnp.bfloat16)
    base_copy.wait()
    other_copy.wait()
    for r in range(0, 2048, 256):
        rs = pl.ds(r, 256)
        a4[rs, :] = jnp.dot(base_v[rs, :], repeat, preferred_element_type=jnp.float32)
        b4[rs, :] = jnp.dot(other_v[rs, :], repeat, preferred_element_type=jnp.float32)
    lane64 = lax.broadcasted_iota(jnp.int32, (64, 128), 1)
    for r in range(0, 2048, 64):
        rs = pl.ds(r, 64)
        av, bv = a4[rs, :], b4[rs, :]
        tail = jnp.where(lane64 == 64, 1.0, 0.0)
        value = jnp.where(lane64 < 32, av + bv, jnp.where(lane64 < 64, av * av + bv * bv, tail))
        terms1[rs, :128] = value.astype(jnp.bfloat16)
    counts_copy.wait()
    for r in range(0, 256, 8):
        rs = pl.ds(r, 8)
        cbf[rs, :] = counts_v[rs, :].astype(jnp.float32).astype(jnp.bfloat16)
    sums = jnp.dot(cbf[...], terms1[:, :128], preferred_element_type=jnp.float32)
    for q in range(2):
        for c in range(2):
            ustage[c, q] = sums[q * 128 + c * 64 : q * 128 + c * 64 + 64, :]

    def make_terms(t, out):
        for r in range(0, 2048, 64):
            rs = pl.ds(r, 64)
            change = mbuf[t, rs, :].astype(jnp.float32) - a4[rs, :]
            out[rs, :128] = (b4[rs, :] * change).astype(jnp.bfloat16)
            out[rs, 128:] = (change * change).astype(jnp.bfloat16)

    mixed_copy(0).wait()
    make_terms(0, terms0)

    pl.semaphore_wait(barrier, len(peers))

    def remote(src, dst, send, recv, target):
        return pltpu.make_async_remote_copy(
            src_ref=src, dst_ref=dst, send_sem=send, recv_sem=recv,
            device_id=target, device_id_type=MESH,
        )

    def u_d2d():
        return remote(ustage.at[1 - core], upart, usend.at[0], urecv.at[0], partner)

    def u_z(d):
        target_zh = ((z + d) % 4) // 2
        return remote(upart.at[target_zh], uz.at[d - 1], usend.at[d], urecv.at[d], at_z(d))

    def u_y(d):
        return remote(uz.at[3], uy.at[d - 1], usend.at[3 + d], urecv.at[3 + d], at_y(d))

    def u_x(d):
        return remote(uy.at[3], ux.at[d - 1], usend.at[6 + d], urecv.at[6 + d], at_x(d))

    def u_fin():
        return remote(ux.at[3], ufin.at[core], usend.at[10], urecv.at[10], partner)

    u_d2d().start()

    def u_stage1():
        u_d2d().wait_recv()
        for q in range(2):
            upart[q] = upart[q] + ustage[core, q]
        for d in (1, 2, 3):
            u_z(d).start()

    def u_stage2():
        for d in (1, 2, 3):
            u_z(d).wait_recv()
        uz[3] = upart[zh] + uz[0] + uz[1] + uz[2]
        for d in (1, 2, 3):
            u_y(d).start()

    def u_stage3():
        for d in (1, 2, 3):
            u_y(d).wait_recv()
        uy[3] = uz[3] + uy[0] + uy[1] + uy[2]
        for d in (1, 2, 3):
            u_x(d).start()

    def u_stage4():
        for d in (1, 2, 3):
            u_x(d).wait_recv()
        ux[3] = uy[3] + ux[0] + ux[1] + ux[2]
        u_fin().start()

    lane128 = lax.broadcasted_iota(jnp.int32, (128, 128), 1)

    def d2d(t):
        s = t // 2
        dx, dy = coords(s)
        return remote(
            stage.at[t, 1 - core], part.at[dx, dy, t % 2], d2d_send.at[t], d2d_recv.at[t], partner
        )

    def multiply(t, dzl, terms):
        result = jnp.dot(cbf[...], terms[...], preferred_element_type=jnp.float32)
        carry = (zl + dzl) // 2
        for q in range(2):
            cross = result[q * 128 : q * 128 + 128, :128]
            square = result[q * 128 : q * 128 + 128, 128:]
            j = (q + zh + carry) % 2
            stage[t, 0, j] = jnp.where(lane128 < 64, cross, pltpu.roll(square, 64, 1))
            stage[t, 1, j] = jnp.where(lane128 < 64, pltpu.roll(cross, 64, 1), square)
        d2d(t).start()

    def compute(s):
        t = 2 * s

        @pl.when(t + AHEAD < 2 * STEPS)
        def _():
            mixed_copy(t + AHEAD).start()
            mixed_copy(t + AHEAD + 1).start()

        mixed_copy(t + 1).wait()
        make_terms(t + 1, terms1)
        multiply(t, 0, terms0)

        @pl.when(t + 2 < 2 * STEPS)
        def _():
            mixed_copy(t + 2).wait()

        make_terms(jnp.minimum(t + 2, 2 * STEPS - 1), terms0)
        multiply(t + 1, 1, terms1)

    def rows(color, h):
        first, count = ROWS[color][h]
        return pl.ds(first, count)

    bufs1 = ((ra0, ra1), (rb0, rb1), (rc0, rc1))

    def message(color, h, dx, dy, direction):
        sem = recv1.at[color, h, dx * 4 + dy]
        return remote(
            part.at[dx, dy, :, :, rows(color, h), :], bufs1[color][h].at[dx, dy],
            send1.at[color, h], sem, axes[color](direction),
        )

    def message_z(h, dx, dy, dz, direction):
        return remote(
            part.at[dx, dy, dz % 2, dz // 2, rows(2, h), :], bufs1[2][h].at[dx, dy, dz - 1],
            send1.at[2, h], recv_c.at[h, dz - 1, dx * 4 + dy], at_z(direction),
        )

    def combine(s):
        dx, dy = coords(s)
        for dzl in range(2):
            t = 2 * s + dzl
            d2d(t).wait_recv()
            for j in range(2):
                part[dx, dy, dzl, j] = part[dx, dy, dzl, j] + stage[t, core, j]
        for color, d in ((0, dx), (1, dy)):

            @pl.when(d == 2)
            def _(color=color):
                message(color, 0, dx, dy, 1).start()
                message(color, 1, dx, dy, 3).start()

            @pl.when(d == 1)
            def _(color=color):
                message(color, 1, dx, dy, 1).start()

            @pl.when(d == 3)
            def _(color=color):
                message(color, 0, dx, dy, 3).start()

        message_z(0, dx, dy, 2, 1).start()
        message_z(1, dx, dy, 2, 3).start()
        message_z(1, dx, dy, 1, 1).start()
        message_z(0, dx, dy, 3, 3).start()

    def forward(s):
        dx, dy = coords(s)
        for color, d in ((0, dx), (1, dy)):
            from_dx, from_dy = (2, dy) if color == 0 else (dx, 2)

            @pl.when(d == 1)
            def _(color=color, from_dx=from_dx, from_dy=from_dy):
                message(color, 0, from_dx, from_dy, 1).wait_recv()
                view = part.at[dx, dy, :, :, rows(color, 0), :]
                view[...] = view[...] + bufs1[color][0][from_dx, from_dy]
                message(color, 0, dx, dy, 1).start()

            @pl.when(d == 3)
            def _(color=color, from_dx=from_dx, from_dy=from_dy):
                message(color, 1, from_dx, from_dy, 3).wait_recv()
                view = part.at[dx, dy, :, :, rows(color, 1), :]
                view[...] = view[...] + bufs1[color][1][from_dx, from_dy]
                message(color, 1, dx, dy, 3).start()

        for h, dz, direction in ((0, 1, 1), (1, 3, 3)):
            message_z(h, dx, dy, 2, direction).wait_recv()
            view = part.at[dx, dy, dz % 2, dz // 2, rows(2, h), :]
            view[...] = view[...] + bufs1[2][h][dx, dy, 1]
            message_z(h, dx, dy, dz, direction).start()

    @pl.loop(0, STEPS + LAG)
    def _(s):
        @pl.when(s < STEPS)
        def _():
            compute(s)

        @pl.when((s >= 1) & (s < STEPS + 1))
        def _():
            combine(s - 1)

        @pl.when(s >= LAG)
        def _():
            forward(s - LAG)

        for at, todo in ((1, u_stage1), (5, u_stage2), (9, u_stage3), (13, u_stage4)):
            @pl.when(s == at)
            def _(todo=todo):
                todo()

    bufs2 = ((q0, q1), (q2, q3), (q4, q5))
    bufs3 = ((v0, v1), (v2, v3), (v4, v5))

    def view2(color, h, d):
        if color == 0:
            return part.at[0, d, :, :, rows(0, h), :]
        if color == 1:
            return part.at[:, 0, d % 2, d // 2, rows(1, h), :]
        return part.at[d, :, 0, 0, rows(2, h), :]

    def finish1(color, h, d):
        buf = bufs1[color][h]
        view = view2(color, h, d)
        if color == 0:
            for side in (1, 3):
                message(0, h, side, d, 1).wait_recv()
            view[...] = view[...] + buf[1, d] + buf[3, d]
        elif color == 1:
            if d == 2:
                for dx in range(4):
                    for side in (1, 3):
                        message(1, h, dx, side, 1).wait_recv()
            view[...] = view[...] + buf[:, 1, d % 2, d // 2] + buf[:, 3, d % 2, d // 2]
        else:
            for dy in range(4):
                for dz in (1, 3):
                    message_z(h, d, dy, dz, 1).wait_recv()
            view[...] = view[...] + buf[d, :, 0] + buf[d, :, 2]

    axis2 = (at_y, at_z, at_x)
    axis3 = (at_z, at_x, at_y)

    def message2(color, h, d, direction):
        return remote(
            view2(color, h, d), bufs2[color][h].at[d - 1],
            send23.at[0, color, h, d - 1], recv2.at[color, h, d - 1], axis2[color](direction),
        )

    def view3(color, h, d):
        if color == 0:
            return part.at[0, 0, d % 2, d // 2, rows(0, h), :]
        if color == 1:
            return part.at[d, 0, 0, 0, rows(1, h), :]
        return part.at[0, d, 0, 0, rows(2, h), :]

    def message3(color, h, d, direction):
        return remote(
            view3(color, h, d), bufs3[color][h].at[d - 1],
            send23.at[1, color, h, d - 1], recv3.at[color, h, d - 1], axis3[color](direction),
        )

    def finish2(color, h, d):
        if d == 2:
            for side in (1, 3):
                message2(color, h, side, 1).wait_recv()
        buf = bufs2[color][h]
        view = view3(color, h, d)
        pick = (d % 2, d // 2) if color == 0 else (d,)
        view[...] = view[...] + buf[(0,) + pick] + buf[(2,) + pick]

    streams = [(color, h) for color in range(3) for h in range(2)]

    def phase(finish, message_of, view_of, bufs):
        for color, h in streams:
            finish(color, h, 2)
            message_of(color, h, 2, 1 if h == 0 else 3).start()
        for color, h in streams:
            d = 3 if h == 0 else 1
            finish(color, h, d)
            message_of(color, h, d, d).start()
        for color, h in streams:
            d = 1 if h == 0 else 3
            finish(color, h, d)
            message_of(color, h, 2, d).wait_recv()
            view = view_of(color, h, d)
            view[...] = view[...] + bufs[color][h][1]
            message_of(color, h, d, d).start()
        for color, h in streams:
            finish(color, h, 0)

    phase(finish1, message2, view2, bufs2)
    phase(finish2, message3, view3, bufs3)

    u_fin().wait_recv()
    ufin[core] = ux[3]
    rolled = []
    for c in range(2):
        sums_c = ufin[c]
        weight = jnp.maximum(sums_c[:, 64:65], 1.0)
        mean = sums_c / (2.0 * weight)
        square_mean = pltpu.roll(sums_c, 96, 1) / (2.0 * weight)
        variance = jnp.maximum(square_mean - mean * mean, 0.25)
        lanes = lax.broadcasted_iota(jnp.int32, (64, 128), 1)
        scaled = jnp.where(lanes < 32, weight * variance, 0.0)
        scaled = scaled + pltpu.roll(scaled, 32, 1)
        scaled = scaled + pltpu.roll(scaled, 64, 1)
        rolled.append(jnp.where(lanes < 64, scaled, 2.0 * scaled))
    divisor = jnp.concatenate(rolled, axis=0)

    for t in range(2 * STEPS):
        d2d(t).wait_send()
    for color in range(2):
        for h in range(2):
            sent = bufs1[color][h].at[:3]
            pltpu.make_async_copy(sent, sent, send1.at[color, h]).wait()
    for h in range(2):
        sent = bufs1[2][h]
        pltpu.make_async_copy(sent, sent, send1.at[2, h]).wait()
    u_d2d().wait_send()
    for d in (1, 2, 3):
        u_z(d).wait_send()
        u_y(d).wait_send()
        u_x(d).wait_send()
    u_fin().wait_send()
    for color, h in streams:
        for d in (1, 2, 3):
            message2(color, h, d, 1).wait_send()
            message3(color, h, d, 1).wait_send()

    for color, h in streams:
        for d in (1, 3):
            message3(color, h, d, 1).wait_recv()
        buf = bufs3[color][h]
        view = view3(color, h, 0)
        view[...] = view[...] + buf[0] + buf[2]

    result = part[0, 0, 0, 0] / divisor
    first_ref[...] = result[:, :64]
    total_ref[...] = pltpu.roll(result, 64, 1)[:, :64]


def shards(base_runs, other_runs, mixed_runs, counts):
    f32, bf16 = jnp.float32, jnp.bfloat16
    dma = pltpu.SemaphoreType.DMA

    def vmem(*shape, dtype=f32):
        return pltpu.VMEM(shape, dtype)

    sizes = [[count for first, count in color] for color in ROWS]
    scratch = [
        vmem(2048, 32, dtype=bf16), vmem(2048, 32, dtype=bf16), vmem(256, 2048, dtype=jnp.int32),
        vmem(256, 2048, dtype=bf16), vmem(2048, 128), vmem(2048, 128),
        vmem(32, 2048, 128, dtype=bf16), vmem(2048, 256, dtype=bf16), vmem(2048, 256, dtype=bf16),
        vmem(32, 2, 2, 128, 128), vmem(4, 4, 2, 2, 128, 128),
    ]
    for color in range(2):
        for h in range(2):
            scratch.append(vmem(4, 4, 2, 2, sizes[color][h], 128))
    for h in range(2):
        scratch.append(vmem(4, 4, 3, sizes[2][h], 128))
    for h in range(2):
        scratch.append(vmem(3, 2, 2, sizes[0][h], 128))
    for color in (1, 2):
        for h in range(2):
            scratch.append(vmem(3, 4, sizes[color][h], 128))
    for color in range(3):
        for h in range(2):
            scratch.append(vmem(3, sizes[color][h], 128))
    scratch += [
        vmem(2, 2, 64, 128), vmem(2, 64, 128), vmem(4, 64, 128), vmem(4, 64, 128),
        vmem(4, 64, 128), vmem(2, 64, 128),
        dma((3,)), dma((32,)), dma((32,)), dma((32,)),
        dma((2, 2, 16)), dma((2, 3, 16)), dma((3, 2)), dma((3, 2, 3)), dma((3, 2, 3)),
        dma((2, 3, 2, 3)), dma((11,)), dma((11,)),
    ]
    any_spec = pl.BlockSpec(memory_space=pl.ANY)
    out = jax.ShapeDtypeStruct((128, 64), f32)
    return pl.pallas_call(
        kernel,
        out_shape=(out, out),
        in_specs=[any_spec] * 4,
        out_specs=(pl.BlockSpec(memory_space=pltpu.VMEM),) * 2,
        scratch_shapes=scratch,
        compiler_params=pltpu.CompilerParams(
            collective_id=0, has_side_effects=True, vmem_limit_bytes=64 * 1024 * 1024 - 65536
        ),
    )(base_runs, other_runs, mixed_runs, counts)


def solution(mesh):
    split = Mesh(mesh.devices.reshape(4, 4, 2, 2, mesh.shape["res"]), AXES)
    every = AXES
    columns = ("x", "y", "zl", "core")
    placed = (P(every, None), P(every, None), P(every, None), P(None, every))
    return jax.shard_map(
        shards,
        mesh=split,
        in_specs=placed,
        out_specs=(P("zh", columns), P("zh", columns)),
        check_vma=False,
    )
```

```python
import functools

import jax
import jax.numpy as jnp
from jax import lax
from jax.experimental import pallas as pl
from jax.experimental.pallas import tpu as pltpu
from jax.sharding import Mesh
from jax.sharding import PartitionSpec as P

MESH = pl.DeviceIdType.MESH
AXES = ("x", "y", "zl", "core", "zh")

ORDER = (
    (2, 2), (2, 1), (1, 2), (2, 3), (3, 2), (1, 1), (1, 3), (3, 1),
    (3, 3), (2, 0), (0, 2), (1, 0), (0, 1), (3, 0), (0, 3), (0, 0),
)
STEPS = len(ORDER)
DX_CODE = sum(dx << (2 * i) for i, (dx, dy) in enumerate(ORDER))
DY_CODE = sum(dy << (2 * i) for i, (dx, dy) in enumerate(ORDER))
DX_LO, DX_HI = DX_CODE & 0xFFFF, DX_CODE >> 16
DY_LO, DY_HI = DY_CODE & 0xFFFF, DY_CODE >> 16
AHEAD = 6
DEPTH = 256
ENTER = 2
COMBINE = 2
ARRIVE = 6
ROWS = (((0, 24), (24, 24)), ((48, 24), (72, 16)), ((88, 16), (104, 24)))


def digit(lo, hi, s):
    code = jnp.where(s < 8, lo, hi)
    return lax.shift_right_logical(code, 2 * (s % 8)) & 3


def coords(s):
    s = jnp.asarray(s, jnp.int32)
    return digit(DX_LO, DX_HI, s), digit(DY_LO, DY_HI, s)


def order_of_work():
    A, B, C = range(3)
    work = []

    def add(time, name, *args):
        work.append((time, len(work), name, args))
        return time

    at = {pair: i for i, pair in enumerate(ORDER)}
    R = ARRIVE
    k, fab, fc = {}, {}, {}
    for pair, i in at.items():
        add(max(i, ENTER), "exchange", i)
        k[pair] = add(max(i, ENTER) + COMBINE, "combine", i)
    for (dx, dy), t in k.items():
        ready = [t]
        if dx in (1, 3):
            ready.append(k[2, dy] + R)
        if dy in (1, 3):
            ready.append(k[dx, 2] + R)
        fab[dx, dy] = max(ready)
        if dx in (1, 3):
            add(fab[dx, dy], "forward", A, 1, dx, (dy,))
        if dy in (1, 3):
            add(fab[dx, dy], "forward", B, 1, dy, (dx,))
        fc[dx, dy] = t + R
        for dz in (1, 3):
            add(fc[dx, dy], "forward", C, 1, dz, (dx, dy))
    a2 = {d: max(k[0, d], fab[1, d] + R, fab[3, d] + R) for d in range(4)}
    b2 = {d: max(k[d, 0], fab[d, 1] + R, fab[d, 3] + R) for d in range(4)}
    c2 = {pair: t + R for pair, t in fc.items()}
    for d in range(4):
        add(a2[d], "arrive", A, 1, (d,))
        if d:
            add(a2[d], "direct", A, 2, d, ())
        add(b2[d], "arrive", B, 1, (d,))
        for dz in (2, 1, 3):
            add(b2[d], "direct", B, 2, dz, (d,))
        for o in range(4):
            add(c2[d, o], "arrive", C, 1, (d, o))
            if d:
                add(c2[d, o], "direct", C, 2, d, (o,))
    a3 = max(a2[0], a2[1] + R, a2[2] + R, a2[3] + R)
    add(a3, "gather", A, 2, ())
    for dz in (2, 1, 3):
        add(a3, "direct", A, 3, dz, ())
    last = [add(a3 + R, "gather", A, 3, ())]
    b3 = {d: b2[d] + R for d in range(4)}
    c3 = {d: max(c2[0, d], *(c2[o, d] + R for o in (1, 2, 3))) for d in range(4)}
    for color, third in ((B, b3), (C, c3)):
        for d in range(4):
            add(third[d], "gather", color, 2, (d,))
            if d:
                add(third[d], "direct", color, 3, d, ())
        last.append(add(max(third[0], *(third[d] + R for d in (1, 2, 3))), "gather", color, 3, ()))
    work.sort()
    return work, last


def kernel(
    base_hbm, other_hbm, mixed_hbm, counts_hbm,
    first_ref, total_ref,
    base_v, other_v, counts_v, cbf, a4, b4, mbuf, stage, part,
    ra0, ra1, rb0, rb1, rc0, rc1,
    qa, qb, qc, va, vb, vc,
    ustage, upart, uz, uy, ux, ufin,
    in_sem, msem, d2d_send, d2d_recv,
    recv1, recv_c, recv2, recv3, send, usend, urecv,
):
    x = lax.axis_index("x")
    y = lax.axis_index("y")
    zl = lax.axis_index("zl")
    core = lax.axis_index("core")
    zh = lax.axis_index("zh")
    z = zh * 2 + zl

    def at_x(d):
        return {"x": (x + d) % 4}

    def at_y(d):
        return {"y": (y + d) % 4}

    def at_z(d):
        target = (z + d) % 4
        return {"zl": target % 2, "zh": target // 2}

    partner = {"core": 1 - core}
    axes = (at_x, at_y, at_z)

    barrier = pltpu.get_barrier_semaphore()
    peers = [partner] + [ax(d) for ax in axes for d in (1, 2, 3)]
    for peer in peers:
        pl.semaphore_signal(barrier, inc=1, device_id=peer, device_id_type=MESH)

    def mixed_copy(t):
        s = t // 2
        dx, dy = coords(s)
        column = ((((x + dx) % 4) * 4 + (y + dy) % 4) * 2 + (zl + t) % 2) * 128
        return pltpu.make_async_copy(
            mixed_hbm.at[:, pl.ds(pl.multiple_of(column, 128), 128)], mbuf.at[t], msem.at[t]
        )

    counts_copy = pltpu.make_async_copy(counts_hbm, counts_v, in_sem.at[0])
    base_copy = pltpu.make_async_copy(base_hbm, base_v, in_sem.at[1])
    other_copy = pltpu.make_async_copy(other_hbm, other_v, in_sem.at[2])
    base_copy.start()
    other_copy.start()
    counts_copy.start()
    for t in range(AHEAD):
        mixed_copy(t).start()

    lane = lax.broadcasted_iota(jnp.int32, (32, 128), 1)
    row = lax.broadcasted_iota(jnp.int32, (32, 128), 0)
    repeat = (lane % 32 == row).astype(jnp.float32).astype(jnp.bfloat16)
    base_copy.wait()
    other_copy.wait()
    for r in range(0, 2048, 256):
        rs = pl.ds(r, 256)
        for wide, runs in ((a4, base_v), (b4, other_v)):
            wide[rs, :] = lax.dot_general(
                runs[:, rs], repeat, (((0,), (0,)), ((), ())), preferred_element_type=jnp.float32
            )
    counts_copy.wait()
    for r in range(0, 256, 16):
        rs = pl.ds(r, 16)
        cbf[rs, :] = counts_v[rs, :].astype(jnp.float32).astype(jnp.bfloat16)

    lane256 = lax.broadcasted_iota(jnp.int32, (DEPTH, 128), 1)

    def moments_of(rs):
        av, bv = a4[rs, :], b4[rs, :]
        tail = jnp.where(lane256 == 64, 1.0, 0.0)
        value = jnp.where(lane256 < 32, av + bv, jnp.where(lane256 < 64, av * av + bv * bv, tail))
        return value.astype(jnp.bfloat16)

    def terms_of(t, rs):
        change = mbuf[t, rs, :].astype(jnp.float32) - a4[rs, :]
        cross = (b4[rs, :] * change).astype(jnp.bfloat16)
        square = (change * change).astype(jnp.bfloat16)
        return jnp.concatenate([cross, square], axis=1)

    def resampled(make):
        total = None
        for r in range(0, 2048, DEPTH):
            piece = jnp.dot(
                cbf[:, r : r + DEPTH], make(pl.ds(r, DEPTH)), preferred_element_type=jnp.float32
            )
            total = piece if total is None else total + piece
        return total

    sums = resampled(moments_of)
    for q in range(2):
        for c in range(2):
            ustage[c, q] = sums[q * 128 + c * 64 : q * 128 + c * 64 + 64, :]


    def remote(src, dst, send, recv, target):
        return pltpu.make_async_remote_copy(
            src_ref=src, dst_ref=dst, send_sem=send, recv_sem=recv,
            device_id=target, device_id_type=MESH,
        )

    def u_d2d():
        return remote(ustage.at[1 - core], upart, usend.at[0], urecv.at[0], partner)

    def u_z(d):
        target_zh = ((z + d) % 4) // 2
        return remote(upart.at[target_zh], uz.at[d - 1], usend.at[d], urecv.at[d], at_z(d))

    def u_y(d):
        return remote(uz.at[3], uy.at[d - 1], usend.at[3 + d], urecv.at[3 + d], at_y(d))

    def u_x(d):
        return remote(uy.at[3], ux.at[d - 1], usend.at[6 + d], urecv.at[6 + d], at_x(d))

    def u_fin():
        return remote(ux.at[3], ufin.at[core], usend.at[10], urecv.at[10], partner)


    def u_stage1():
        u_d2d().wait_recv()
        for q in range(2):
            upart[q] = upart[q] + ustage[core, q]
        for d in (1, 2, 3):
            u_z(d).start()

    def u_stage2():
        for d in (1, 2, 3):
            u_z(d).wait_recv()
        uz[3] = upart[zh] + uz[0] + uz[1] + uz[2]
        for d in (1, 2, 3):
            u_y(d).start()

    def u_stage3():
        for d in (1, 2, 3):
            u_y(d).wait_recv()
        uy[3] = uz[3] + uy[0] + uy[1] + uy[2]
        for d in (1, 2, 3):
            u_x(d).start()

    def u_stage4():
        for d in (1, 2, 3):
            u_x(d).wait_recv()
        ux[3] = uy[3] + ux[0] + ux[1] + ux[2]
        u_fin().start()

    lane128 = lax.broadcasted_iota(jnp.int32, (128, 128), 1)

    def d2d(t):
        dx, dy = ORDER[t // 2]
        return remote(
            stage.at[t, 1 - core], part.at[dx, dy, t % 2], d2d_send, d2d_recv.at[t], partner
        )

    def multiply(t, dzl):
        result = resampled(lambda rs: terms_of(t, rs))
        carry = (zl + dzl) // 2
        for q in range(2):
            cross = result[q * 128 : q * 128 + 128, :128]
            square = result[q * 128 : q * 128 + 128, 128:]
            j = (q + zh + carry) % 2
            stage[t, 0, j] = jnp.where(lane128 < 64, cross, pltpu.roll(square, 64, 1))
            stage[t, 1, j] = jnp.where(lane128 < 64, pltpu.roll(cross, 64, 1), square)

    def compute(s):
        t = 2 * s

        @pl.when(t + AHEAD < 2 * STEPS)
        def _():
            mixed_copy(t + AHEAD).start()
            mixed_copy(t + AHEAD + 1).start()

        mixed_copy(t).wait()
        mixed_copy(t + 1).wait()
        multiply(t, 0)
        multiply(t + 1, 1)

    bufs = {
        1: ((ra0, ra1), (rb0, rb1), (rc0, rc1)),
        2: ((qa,), (qb,), (qc,)),
        3: ((va,), (vb,), (vc,)),
    }

    def view(color, phase, d, other, h):
        if phase == 1:
            where = ((d, *other), (*other, d), (*other, d % 2, d // 2))[color]
        elif phase == 2:
            where = ((0, d), (*other, 0, d % 2, d // 2), (d, *other, 0, 0))[color]
        else:
            where = ((0, 0, d % 2, d // 2), (d, 0, 0, 0), (0, d, 0, 0))[color]
        first, count = ROWS[color][0] if phase > 1 else ROWS[color][h]
        if phase > 1:
            count += ROWS[color][1][1]
        full = (slice(None),) * (4 - len(where))
        return part.at[(*where, *full, pl.ds(first, count))]

    def message(color, phase, d, other, h, direction):
        flat = sum(o * 4**i for i, o in enumerate(other))
        if phase == 1:
            sem = recv_c.at[h, d - 1, flat] if color == 2 else recv1.at[color, h, d - 1, flat]
        elif phase == 2:
            sem = recv2.at[color, d - 1, flat]
        else:
            sem = recv3.at[color, d - 1]
        return remote(
            view(color, phase, d, other, h), bufs[phase][color][h].at[(d - 1, *other)],
            send.at[phase - 1, color, h], sem, axes[(color + phase - 1) % 3](direction),
        )

    def launch(color, phase, d, other):
        if d != 3:
            h = 1 if d == 1 else 0
            message(color, phase, d, other, h, 1).start()
        if d != 1:
            h = 0 if d == 3 else 1
            message(color, phase, d, other, h, 3).start()

    def forward(color, phase, d, other):
        h = 0 if d == 1 else 1
        message(color, phase, 2, other, h, d).wait_recv()
        here = view(color, phase, d, other, h)
        here[...] = here[...] + bufs[phase][color][h][(1, *other)]
        message(color, phase, d, other, h, d).start()

    def arrive(color, phase, other):
        for h in range(2):
            for d in (1, 3):
                message(color, phase, d, other, h, d).wait_recv()
            buf = bufs[phase][color][h]
            here = view(color, phase, 0, other, h)
            here[...] = here[...] + buf[(0, *other)] + buf[(2, *other)]

    def direct(color, phase, d, other):
        message(color, phase, d, other, 0, d).start()

    def gather(color, phase, other):
        for d in (1, 2, 3):
            message(color, phase, d, other, 0, d).wait_recv()
        buf = bufs[phase][color][0]
        here = view(color, phase, 0, other, 0)
        here[...] = (here[...] + buf[(0, *other)]) + (buf[(1, *other)] + buf[(2, *other)])

    def exchange(i):
        d2d(2 * i).start()
        d2d(2 * i + 1).start()

    def combine(i):
        dx, dy = ORDER[i]
        for dzl in range(2):
            d2d(2 * i + dzl).wait_recv()
            for j in range(2):
                part[dx, dy, dzl, j] = part[dx, dy, dzl, j] + stage[2 * i + dzl, core, j]
        if dx:
            launch(0, 1, dx, (dy,))
        if dy:
            launch(1, 1, dy, (dx,))
        for dz in (2, 1, 3):
            launch(2, 1, dz, (dx, dy))

    def enter():
        pl.semaphore_wait(barrier, len(peers))
        u_d2d().start()

    work, last = order_of_work()
    does = dict(exchange=exchange, combine=combine, launch=launch, forward=forward, arrive=arrive, direct=direct, gather=gather)
    todo = [(time, count, functools.partial(does[name], *args)) for time, count, name, args in work]
    todo.append((ENTER, -1, enter))
    for i, u_stage in enumerate((u_stage1, u_stage2, u_stage3, u_stage4)):
        todo.append((ENTER + 2 + 5 * i, -1, u_stage))
    todo.sort(key=lambda item: item[:2])
    final = [item for item in todo if item[0] >= min(last)]
    todo = todo[: len(todo) - len(final)]

    @pl.loop(0, STEPS)
    def _(s):
        compute(s)
        for quarter in range(0, STEPS, 4):

            @pl.when(s // 4 == quarter // 4)
            def _(quarter=quarter):
                for step in range(quarter, quarter + 4):
                    now = [run for time, count, run in todo if step - 1 < time <= step]
                    if now:

                        @pl.when(s == step)
                        def _(now=now):
                            for run in now:
                                run()

    for time, count, run in todo:
        if time > STEPS - 1:
            run()

    u_fin().wait_recv()
    ufin[core] = ux[3]
    rolled = []
    for c in range(2):
        sums_c = ufin[c]
        weight = jnp.maximum(sums_c[:, 64:65], 1.0)
        mean = sums_c / (2.0 * weight)
        square_mean = pltpu.roll(sums_c, 96, 1) / (2.0 * weight)
        variance = jnp.maximum(square_mean - mean * mean, 0.25)
        lanes = lax.broadcasted_iota(jnp.int32, (64, 128), 1)
        scaled = jnp.where(lanes < 32, weight * variance, 0.0)
        scaled = scaled + pltpu.roll(scaled, 32, 1)
        scaled = scaled + pltpu.roll(scaled, 64, 1)
        rolled.append(jnp.where(lanes < 64, scaled, 2.0 * scaled))
    divisor = jnp.concatenate(rolled, axis=0)

    def all_left(ref, sem):
        pltpu.make_async_copy(ref, ref, sem).wait()

    all_left(stage.at[:, 0], d2d_send)
    u_d2d().wait_send()
    for d in (1, 2, 3):
        u_z(d).wait_send()
        u_y(d).wait_send()
        u_x(d).wait_send()
    u_fin().wait_send()

    for time, count, run in final:
        run()
    for phase, colors in bufs.items():
        for color in range(3):
            for h, buf in enumerate(colors[color]):
                all_left(buf, send.at[phase - 1, color, h])

    result = part[0, 0, 0, 0] / divisor
    result = result.T
    first_ref[...] = result[:64]
    total_ref[...] = result[64:]


def shards(base_runs, other_runs, mixed_runs, counts):
    f32, bf16 = jnp.float32, jnp.bfloat16
    dma = pltpu.SemaphoreType.DMA

    def vmem(*shape, dtype=f32):
        return pltpu.VMEM(shape, dtype)

    sizes = [[count for first, count in color] for color in ROWS]
    scratch = [
        vmem(32, 2048, dtype=bf16), vmem(32, 2048, dtype=bf16), vmem(256, 2048, dtype=jnp.int32),
        vmem(256, 2048, dtype=bf16), vmem(2048, 128), vmem(2048, 128),
        vmem(32, 2048, 128, dtype=bf16),
        vmem(32, 2, 2, 128, 128), vmem(4, 4, 2, 2, 128, 128),
    ]
    inside = (
        ((3, 4, 2, 2), (3, 4, 2, 2), (3, 4, 4)),
        ((3, 2, 2), (3, 4), (3, 4)),
        ((3,), (3,), (3,)),
    )
    for phase, shapes in enumerate(inside, 1):
        for color in range(3):
            for count in sizes[color] if phase == 1 else [sum(sizes[color])]:
                scratch.append(vmem(*shapes[color], count, 128))
    scratch += [
        vmem(2, 2, 64, 128), vmem(2, 64, 128), vmem(4, 64, 128), vmem(4, 64, 128),
        vmem(4, 64, 128), vmem(2, 64, 128),
        dma((3,)), dma((32,)), dma, dma((32,)),
        dma((2, 2, 3, 4)), dma((2, 3, 16)), dma((3, 3, 4)), dma((3, 3)), dma((3, 3, 2)),
        dma((11,)), dma((11,)),
    ]
    any_spec = pl.BlockSpec(memory_space=pl.ANY)
    out = jax.ShapeDtypeStruct((64, 128), f32)
    first_order, total_order = pl.pallas_call(
        kernel,
        out_shape=(out, out),
        in_specs=[any_spec] * 4,
        out_specs=(pl.BlockSpec(memory_space=pltpu.VMEM),) * 2,
        scratch_shapes=scratch,
        compiler_params=pltpu.CompilerParams(
            collective_id=0, has_side_effects=True, vmem_limit_bytes=64 * 1024 * 1024 - 65536
        ),
    )(base_runs.T, other_runs.T, mixed_runs, counts)
    return first_order.T, total_order.T


def solution(mesh):
    split = Mesh(mesh.devices.reshape(4, 4, 2, 2, mesh.shape["res"]), AXES)
    every = AXES
    columns = ("x", "y", "zl", "core")
    placed = (P(every, None), P(every, None), P(every, None), P(None, every))
    return jax.shard_map(
        shards,
        mesh=split,
        in_specs=placed,
        out_specs=(P("zh", columns), P("zh", columns)),
        check_vma=False,
    )
```

```python
import functools

import jax
import jax.numpy as jnp
from jax import lax
from jax.experimental import pallas as pl
from jax.experimental.pallas import tpu as pltpu
from jax.sharding import Mesh
from jax.sharding import PartitionSpec as P

MESH = pl.DeviceIdType.MESH
AXES = ("x", "y", "zl", "core", "zh")

ORDER = (
    (2, 2), (2, 1), (1, 2), (2, 3), (3, 2), (1, 1), (1, 3), (3, 1),
    (3, 3), (2, 0), (0, 2), (1, 0), (0, 1), (3, 0), (0, 3), (0, 0),
)
STEPS = len(ORDER)
DX_CODE = sum(dx << (2 * i) for i, (dx, dy) in enumerate(ORDER))
DY_CODE = sum(dy << (2 * i) for i, (dx, dy) in enumerate(ORDER))
DX_LO, DX_HI = DX_CODE & 0xFFFF, DX_CODE >> 16
DY_LO, DY_HI = DY_CODE & 0xFFFF, DY_CODE >> 16
AHEAD = 6
DEPTH = 256
ENTER = 2
COMBINE = 2
ARRIVE = 6
DIRECT = (2,)
ROWS = (((0, 24), (24, 24)), ((48, 24), (72, 16)), ((88, 16), (104, 24)))


def digit(lo, hi, s):
    code = jnp.where(s < 8, lo, hi)
    return lax.shift_right_logical(code, 2 * (s % 8)) & 3


def coords(s):
    s = jnp.asarray(s, jnp.int32)
    return digit(DX_LO, DX_HI, s), digit(DY_LO, DY_HI, s)


def order_of_work():
    A, B, C = range(3)
    work = []

    def add(time, name, *args):
        work.append((time, len(work), name, args))
        return time

    at = {pair: i for i, pair in enumerate(ORDER)}
    R = ARRIVE
    k, fab, fc = {}, {}, {}
    for pair, i in at.items():
        add(max(i, ENTER), "exchange", i)
        k[pair] = add(max(i, ENTER) + COMBINE, "combine", i)
    for (dx, dy), t in k.items():
        for color, d, other, across in ((A, dx, dy, (2, dy)), (B, dy, dx, (dx, 2))):
            fab[color, dx, dy] = t
            if d in (1, 3) and color not in DIRECT:
                fab[color, dx, dy] = add(max(t, k[across] + R), "forward", color, 1, d, (other,))
        fc[dx, dy] = t
        if C not in DIRECT:
            fc[dx, dy] = t + R
            for dz in (1, 3):
                add(fc[dx, dy], "forward", C, 1, dz, (dx, dy))
    a2 = {d: max(k[0, d], *(fab[A, o, d] + R for o in (1, 2, 3))) for d in range(4)}
    b2 = {d: max(k[d, 0], *(fab[B, d, o] + R for o in (1, 2, 3))) for d in range(4)}
    reach = {color: "gather" if color in DIRECT else "arrive" for color in range(3)}
    c2 = {pair: t + R for pair, t in fc.items()}
    for d in range(4):
        add(a2[d], reach[A], A, 1, (d,))
        if d:
            add(a2[d], "direct", A, 2, d, ())
        add(b2[d], reach[B], B, 1, (d,))
        for dz in (2, 1, 3):
            add(b2[d], "direct", B, 2, dz, (d,))
        for o in range(4):
            add(c2[d, o], reach[C], C, 1, (d, o))
            if d:
                add(c2[d, o], "direct", C, 2, d, (o,))
    a3 = max(a2[0], a2[1] + R, a2[2] + R, a2[3] + R)
    add(a3, "gather", A, 2, ())
    for dz in (2, 1, 3):
        add(a3, "direct", A, 3, dz, ())
    last = [add(a3 + R, "gather", A, 3, ())]
    b3 = {d: b2[d] + R for d in range(4)}
    c3 = {d: max(c2[0, d], *(c2[o, d] + R for o in (1, 2, 3))) for d in range(4)}
    for color, third in ((B, b3), (C, c3)):
        for d in range(4):
            add(third[d], "gather", color, 2, (d,))
            if d:
                add(third[d], "direct", color, 3, d, ())
        last.append(add(max(third[0], *(third[d] + R for d in (1, 2, 3))), "gather", color, 3, ()))
    work.sort()
    return work, last


def kernel(
    base_hbm, other_hbm, mixed_hbm, counts_hbm,
    sums_ref, divisor_ref,
    base_v, other_v, counts_v, cbf, a4, b4, mbuf, stage, part, bufs,
    ustage, upart, uz, uy, ux, ufin,
    in_sem, msem, d2d_send, d2d_recv,
    recv1, recv_c, recv2, recv3, send, usend, urecv,
):
    x = lax.axis_index("x")
    y = lax.axis_index("y")
    zl = lax.axis_index("zl")
    core = lax.axis_index("core")
    zh = lax.axis_index("zh")
    z = zh * 2 + zl

    def at_x(d):
        return {"x": (x + d) % 4}

    def at_y(d):
        return {"y": (y + d) % 4}

    def at_z(d):
        target = (z + d) % 4
        return {"zl": target % 2, "zh": target // 2}

    partner = {"core": 1 - core}
    axes = (at_x, at_y, at_z)

    barrier = pltpu.get_barrier_semaphore()
    peers = [partner] + [ax(d) for ax in axes for d in (1, 2, 3)]
    for peer in peers:
        pl.semaphore_signal(barrier, inc=1, device_id=peer, device_id_type=MESH)

    def mixed_copy(t):
        s = t // 2
        dx, dy = coords(s)
        column = ((((x + dx) % 4) * 4 + (y + dy) % 4) * 2 + (zl + t) % 2) * 128
        return pltpu.make_async_copy(
            mixed_hbm.at[:, pl.ds(pl.multiple_of(column, 128), 128)], mbuf.at[t], msem.at[t]
        )

    counts_copy = pltpu.make_async_copy(counts_hbm, counts_v, in_sem.at[0])
    base_copy = pltpu.make_async_copy(base_hbm, base_v, in_sem.at[1])
    other_copy = pltpu.make_async_copy(other_hbm, other_v, in_sem.at[2])
    base_copy.start()
    other_copy.start()
    counts_copy.start()
    for t in range(AHEAD):
        mixed_copy(t).start()

    lane = lax.broadcasted_iota(jnp.int32, (32, 128), 1)
    row = lax.broadcasted_iota(jnp.int32, (32, 128), 0)
    repeat = (lane % 32 == row).astype(jnp.float32).astype(jnp.bfloat16)
    base_copy.wait()
    other_copy.wait()
    for r in range(0, 2048, 256):
        rs = pl.ds(r, 256)
        for wide, runs in ((a4, base_v), (b4, other_v)):
            wide[rs, :] = lax.dot_general(
                runs[:, rs], repeat, (((0,), (0,)), ((), ())), preferred_element_type=jnp.float32
            )
    counts_copy.wait()
    for r in range(0, 256, 16):
        rs = pl.ds(r, 16)
        cbf[rs, :] = counts_v[rs, :].astype(jnp.float32).astype(jnp.bfloat16)

    lane256 = lax.broadcasted_iota(jnp.int32, (DEPTH, 128), 1)

    def moments_of(rs):
        av, bv = a4[rs, :], b4[rs, :]
        tail = jnp.where(lane256 == 64, 1.0, 0.0)
        value = jnp.where(lane256 < 32, av + bv, jnp.where(lane256 < 64, av * av + bv * bv, tail))
        return value.astype(jnp.bfloat16)

    def terms_of(t, rs):
        change = mbuf[t, rs, :].astype(jnp.float32) - a4[rs, :]
        cross = (b4[rs, :] * change).astype(jnp.bfloat16)
        square = (change * change).astype(jnp.bfloat16)
        return jnp.concatenate([cross, square], axis=1)

    def resampled(make):
        total = None
        for r in range(0, 2048, DEPTH):
            piece = jnp.dot(
                cbf[:, r : r + DEPTH], make(pl.ds(r, DEPTH)), preferred_element_type=jnp.float32
            )
            total = piece if total is None else total + piece
        return total

    sums = resampled(moments_of)
    for q in range(2):
        for c in range(2):
            ustage[c, q] = sums[q * 128 + c * 64 : q * 128 + c * 64 + 64, :]


    def remote(src, dst, send, recv, target):
        return pltpu.make_async_remote_copy(
            src_ref=src, dst_ref=dst, send_sem=send, recv_sem=recv,
            device_id=target, device_id_type=MESH,
        )

    def u_d2d():
        return remote(ustage.at[1 - core], upart, usend.at[0], urecv.at[0], partner)

    def u_z(d):
        target_zh = ((z + d) % 4) // 2
        return remote(upart.at[target_zh], uz.at[d - 1], usend.at[d], urecv.at[d], at_z(d))

    def u_y(d):
        return remote(uz.at[3], uy.at[d - 1], usend.at[3 + d], urecv.at[3 + d], at_y(d))

    def u_x(d):
        return remote(uy.at[3], ux.at[d - 1], usend.at[6 + d], urecv.at[6 + d], at_x(d))

    def u_fin():
        return remote(ux.at[3], ufin.at[core], usend.at[10], urecv.at[10], partner)


    def u_stage1():
        u_d2d().wait_recv()
        for q in range(2):
            upart[q] = upart[q] + ustage[core, q]
        for d in (1, 2, 3):
            u_z(d).start()

    def u_stage2():
        for d in (1, 2, 3):
            u_z(d).wait_recv()
        uz[3] = upart[zh] + uz[0] + uz[1] + uz[2]
        for d in (1, 2, 3):
            u_y(d).start()

    def u_stage3():
        for d in (1, 2, 3):
            u_y(d).wait_recv()
        uy[3] = uz[3] + uy[0] + uy[1] + uy[2]
        for d in (1, 2, 3):
            u_x(d).start()

    def u_stage4():
        for d in (1, 2, 3):
            u_x(d).wait_recv()
        ux[3] = uy[3] + ux[0] + ux[1] + ux[2]
        u_fin().start()

    lane128 = lax.broadcasted_iota(jnp.int32, (128, 128), 1)

    def d2d(t):
        dx, dy = ORDER[t // 2]
        return remote(
            stage.at[t, 1 - core], part.at[dx, dy, t % 2], d2d_send, d2d_recv.at[t], partner
        )

    def multiply(t, dzl):
        result = resampled(lambda rs: terms_of(t, rs))
        carry = (zl + dzl) // 2
        for q in range(2):
            cross = result[q * 128 : q * 128 + 128, :128]
            square = result[q * 128 : q * 128 + 128, 128:]
            j = (q + zh + carry) % 2
            stage[t, 0, j] = jnp.where(lane128 < 64, cross, pltpu.roll(square, 64, 1))
            stage[t, 1, j] = jnp.where(lane128 < 64, pltpu.roll(cross, 64, 1), square)

    def compute(s):
        t = 2 * s

        @pl.when(t + AHEAD < 2 * STEPS)
        def _():
            mixed_copy(t + AHEAD).start()
            mixed_copy(t + AHEAD + 1).start()

        mixed_copy(t).wait()
        mixed_copy(t + 1).wait()
        multiply(t, 0)
        multiply(t + 1, 1)

    def view(color, phase, d, other, h):
        if phase == 1:
            where = ((d, *other), (*other, d), (*other, d % 2, d // 2))[color]
        elif phase == 2:
            where = ((0, d), (*other, 0, d % 2, d // 2), (d, *other, 0, 0))[color]
        else:
            where = ((0, 0, d % 2, d // 2), (d, 0, 0, 0), (0, d, 0, 0))[color]
        first, count = ROWS[color][h]
        if len(bufs[phase][color]) == 1:
            count += ROWS[color][1][1]
        full = (slice(None),) * (4 - len(where))
        return part.at[(*where, *full, pl.ds(first, count))]

    def message(color, phase, d, other, h, direction):
        flat = sum(o * 4**i for i, o in enumerate(other))
        if phase == 1:
            sem = recv_c.at[h, d - 1, flat] if color == 2 else recv1.at[color, h, d - 1, flat]
        elif phase == 2:
            sem = recv2.at[color, d - 1, flat]
        else:
            sem = recv3.at[color, d - 1]
        return remote(
            view(color, phase, d, other, h), bufs[phase][color][h].at[(d - 1, *other)],
            send.at[phase - 1, color, h], sem, axes[(color + phase - 1) % 3](direction),
        )

    def launch(color, phase, d, other):
        if d != 3:
            h = 1 if d == 1 else 0
            message(color, phase, d, other, h, 1).start()
        if d != 1:
            h = 0 if d == 3 else 1
            message(color, phase, d, other, h, 3).start()

    def forward(color, phase, d, other):
        h = 0 if d == 1 else 1
        message(color, phase, 2, other, h, d).wait_recv()
        here = view(color, phase, d, other, h)
        here[...] = here[...] + bufs[phase][color][h][(1, *other)]
        message(color, phase, d, other, h, d).start()

    def arrive(color, phase, other):
        for h in range(2):
            for d in (1, 3):
                message(color, phase, d, other, h, d).wait_recv()
            buf = bufs[phase][color][h]
            here = view(color, phase, 0, other, h)
            here[...] = here[...] + buf[(0, *other)] + buf[(2, *other)]

    def direct(color, phase, d, other):
        for h in range(len(bufs[phase][color])):
            message(color, phase, d, other, h, d).start()

    def gather(color, phase, other):
        for h, buf in enumerate(bufs[phase][color]):
            for d in (1, 2, 3):
                message(color, phase, d, other, h, d).wait_recv()
            here = view(color, phase, 0, other, h)
            here[...] = (here[...] + buf[(0, *other)]) + (buf[(1, *other)] + buf[(2, *other)])

    def exchange(i):
        d2d(2 * i).start()
        d2d(2 * i + 1).start()

    def combine(i):
        dx, dy = ORDER[i]
        for dzl in range(2):
            d2d(2 * i + dzl).wait_recv()
            for j in range(2):
                part[dx, dy, dzl, j] = part[dx, dy, dzl, j] + stage[2 * i + dzl, core, j]
        leave = [direct if color in DIRECT else launch for color in range(3)]
        if dx:
            leave[0](0, 1, dx, (dy,))
        if dy:
            leave[1](1, 1, dy, (dx,))
        for dz in (2, 1, 3):
            leave[2](2, 1, dz, (dx, dy))

    def enter():
        pl.semaphore_wait(barrier, len(peers))
        u_d2d().start()

    work, last = order_of_work()
    does = dict(exchange=exchange, combine=combine, launch=launch, forward=forward, arrive=arrive, direct=direct, gather=gather)
    todo = [(time, count, functools.partial(does[name], *args)) for time, count, name, args in work]
    todo.append((ENTER, -1, enter))
    for i, u_stage in enumerate((u_stage1, u_stage2, u_stage3, u_stage4)):
        todo.append((ENTER + 2 + 5 * i, -1, u_stage))
    todo.sort(key=lambda item: item[:2])
    final = [item for item in todo if item[0] >= min(last)]
    todo = todo[: len(todo) - len(final)]

    @pl.loop(0, STEPS)
    def _(s):
        compute(s)
        for quarter in range(0, STEPS, 4):

            @pl.when(s // 4 == quarter // 4)
            def _(quarter=quarter):
                for step in range(quarter, quarter + 4):
                    now = [run for time, count, run in todo if step - 1 < time <= step]
                    if now:

                        @pl.when(s == step)
                        def _(now=now):
                            for run in now:
                                run()

    for time, count, run in todo:
        if time > STEPS - 1:
            run()

    u_fin().wait_recv()
    ufin[core] = ux[3]
    rolled = []
    for c in range(2):
        sums_c = ufin[c]
        weight = jnp.maximum(sums_c[:, 64:65], 1.0)
        mean = sums_c / (2.0 * weight)
        square_mean = pltpu.roll(sums_c, 96, 1) / (2.0 * weight)
        variance = jnp.maximum(square_mean - mean * mean, 0.25)
        lanes = lax.broadcasted_iota(jnp.int32, (64, 128), 1)
        scaled = jnp.where(lanes < 32, weight * variance, 0.0)
        scaled = scaled + pltpu.roll(scaled, 32, 1)
        scaled = scaled + pltpu.roll(scaled, 64, 1)
        rolled.append(jnp.where(lanes < 64, scaled, 2.0 * scaled))
    divisor = jnp.concatenate(rolled, axis=0)

    def all_left(ref, sem):
        pltpu.make_async_copy(ref, ref, sem).wait()

    all_left(stage.at[:, 0], d2d_send)
    u_d2d().wait_send()
    for d in (1, 2, 3):
        u_z(d).wait_send()
        u_y(d).wait_send()
        u_x(d).wait_send()
    u_fin().wait_send()

    for time, count, run in final:
        run()
    for phase, colors in bufs.items():
        for color in range(3):
            for h, buf in enumerate(colors[color]):
                all_left(buf, send.at[phase - 1, color, h])

    sums_ref[...] = part[0, 0, 0, 0].T
    divisor_ref[...] = divisor.T


def shards(base_runs, other_runs, mixed_runs, counts):
    f32, bf16 = jnp.float32, jnp.bfloat16
    dma = pltpu.SemaphoreType.DMA

    def vmem(*shape, dtype=f32):
        return pltpu.VMEM(shape, dtype)

    sizes = [[count for first, count in color] for color in ROWS]
    scratch = [
        vmem(32, 2048, dtype=bf16), vmem(32, 2048, dtype=bf16), vmem(256, 2048, dtype=jnp.int32),
        vmem(256, 2048, dtype=bf16), vmem(2048, 128), vmem(2048, 128),
        vmem(32, 2048, 128, dtype=bf16),
        vmem(32, 2, 2, 128, 128), vmem(4, 4, 2, 2, 128, 128),
    ]
    inside = (
        ((3, 4, 2, 2), (3, 4, 2, 2), (3, 4, 4)),
        ((3, 2, 2), (3, 4), (3, 4)),
        ((3,), (3,), (3,)),
    )
    scratch.append({
        phase: [
            [
                vmem(*shapes[color], count, 128)
                for count in ([sum(sizes[color])] if phase > 1 or color in DIRECT else sizes[color])
            ]
            for color in range(3)
        ]
        for phase, shapes in enumerate(inside, 1)
    })
    scratch += [
        vmem(2, 2, 64, 128), vmem(2, 64, 128), vmem(4, 64, 128), vmem(4, 64, 128),
        vmem(4, 64, 128), vmem(2, 64, 128),
        dma((3,)), dma((32,)), dma, dma((32,)),
        dma((2, 2, 3, 4)), dma((2, 3, 16)), dma((3, 3, 4)), dma((3, 3)), dma((3, 3, 2)),
        dma((11,)), dma((11,)),
    ]
    any_spec = pl.BlockSpec(memory_space=pl.ANY)
    out = jax.ShapeDtypeStruct((128, 128), f32)
    sums, divisor = pl.pallas_call(
        kernel,
        out_shape=(out, out),
        in_specs=[any_spec] * 4,
        out_specs=(pl.BlockSpec(memory_space=pltpu.VMEM),) * 2,
        scratch_shapes=scratch,
        compiler_params=pltpu.CompilerParams(
            collective_id=0, has_side_effects=True, vmem_limit_bytes=64 * 1024 * 1024 - 65536
        ),
    )(base_runs.T, other_runs.T, mixed_runs, counts)
    return (sums[:64] / divisor[:64]).T, (sums[64:] / divisor[64:]).T


def solution(mesh):
    split = Mesh(mesh.devices.reshape(4, 4, 2, 2, mesh.shape["res"]), AXES)
    every = AXES
    columns = ("x", "y", "zl", "core")
    placed = (P(every, None), P(every, None), P(every, None), P(None, every))
    return jax.shard_map(
        shards,
        mesh=split,
        in_specs=placed,
        out_specs=(P("zh", columns), P("zh", columns)),
        check_vma=False,
    )
```

```python
import functools

import jax
import jax.numpy as jnp
from jax import lax
from jax.experimental import pallas as pl
from jax.experimental.pallas import tpu as pltpu
from jax.sharding import Mesh
from jax.sharding import PartitionSpec as P

MESH = pl.DeviceIdType.MESH
AXES = ("x", "y", "zl", "core", "zh")

ORDER = (
    (2, 2), (2, 1), (1, 2), (2, 3), (3, 2), (1, 1), (1, 3), (3, 1),
    (3, 3), (2, 0), (0, 2), (1, 0), (0, 1), (3, 0), (0, 3), (0, 0),
)
STEPS = len(ORDER)
DX_CODE = sum(dx << (2 * i) for i, (dx, dy) in enumerate(ORDER))
DY_CODE = sum(dy << (2 * i) for i, (dx, dy) in enumerate(ORDER))
DX_LO, DX_HI = DX_CODE & 0xFFFF, DX_CODE >> 16
DY_LO, DY_HI = DY_CODE & 0xFFFF, DY_CODE >> 16
AHEAD = 6
DEPTH = 256
ENTER = 2
COMBINE = 2
ARRIVE = 6
DIRECT = (2,)
ROWS = (((0, 24), (24, 24)), ((48, 24), (72, 16)), ((88, 16), (104, 24)))


def digit(lo, hi, s):
    code = jnp.where(s < 8, lo, hi)
    return lax.shift_right_logical(code, 2 * (s % 8)) & 3


def coords(s):
    s = jnp.asarray(s, jnp.int32)
    return digit(DX_LO, DX_HI, s), digit(DY_LO, DY_HI, s)


def order_of_work():
    A, B, C = range(3)
    work = []

    def add(time, name, *args):
        work.append((time, len(work), name, args))
        return time

    at = {pair: i for i, pair in enumerate(ORDER)}
    R = ARRIVE
    k, fab, fc = {}, {}, {}
    for pair, i in at.items():
        add(max(i, ENTER), "exchange", i)
        k[pair] = add(max(i, ENTER) + COMBINE, "combine", i)
    for (dx, dy), t in k.items():
        for color, d, other, across in ((A, dx, dy, (2, dy)), (B, dy, dx, (dx, 2))):
            fab[color, dx, dy] = t
            if d in (1, 3) and color not in DIRECT:
                fab[color, dx, dy] = add(max(t, k[across] + R), "forward", color, 1, d, (other,))
        fc[dx, dy] = t
        if C not in DIRECT:
            fc[dx, dy] = t + R
            for dz in (1, 3):
                add(fc[dx, dy], "forward", C, 1, dz, (dx, dy))
    a2 = {d: max(k[0, d], *(fab[A, o, d] + R for o in (1, 2, 3))) for d in range(4)}
    b2 = {d: max(k[d, 0], *(fab[B, d, o] + R for o in (1, 2, 3))) for d in range(4)}
    reach = {color: "gather" if color in DIRECT else "arrive" for color in range(3)}
    c2 = {pair: t + R for pair, t in fc.items()}
    for d in range(4):
        add(a2[d], reach[A], A, 1, (d,))
        if d:
            add(a2[d], "direct", A, 2, d, ())
        add(b2[d], reach[B], B, 1, (d,))
        for dz in (2, 1, 3):
            add(b2[d], "direct", B, 2, dz, (d,))
        for o in range(4):
            add(c2[d, o], reach[C], C, 1, (d, o))
            if d:
                add(c2[d, o], "direct", C, 2, d, (o,))
    a3 = max(a2[0], a2[1] + R, a2[2] + R, a2[3] + R)
    add(a3, "gather", A, 2, ())
    for dz in (2, 1, 3):
        add(a3, "direct", A, 3, dz, ())
    last = [add(a3 + R, "gather", A, 3, ())]
    b3 = {d: b2[d] + R for d in range(4)}
    c3 = {d: max(c2[0, d], *(c2[o, d] + R for o in (1, 2, 3))) for d in range(4)}
    for color, third in ((B, b3), (C, c3)):
        for d in range(4):
            add(third[d], "gather", color, 2, (d,))
            if d:
                add(third[d], "direct", color, 3, d, ())
        last.append(add(max(third[0], *(third[d] + R for d in (1, 2, 3))), "gather", color, 3, ()))
    work.sort()
    return work, last


def kernel(
    base_hbm, other_hbm, mixed_hbm, counts_hbm,
    sums_ref, divisor_ref,
    base_v, other_v, counts_v, cbf, a4, b4, mbuf, stage, part, bufs,
    ustage, upart, uz, uy, ux, ufin,
    in_sem, msem, d2d_send, d2d_recv,
    recv1, recv_c, recv2, recv3, send, usend, urecv,
):
    x = lax.axis_index("x")
    y = lax.axis_index("y")
    zl = lax.axis_index("zl")
    core = lax.axis_index("core")
    zh = lax.axis_index("zh")
    z = zh * 2 + zl

    def at_x(d):
        return {"x": (x + d) % 4}

    def at_y(d):
        return {"y": (y + d) % 4}

    def at_z(d):
        target = (z + d) % 4
        return {"zl": target % 2, "zh": target // 2}

    partner = {"core": 1 - core}
    axes = (at_x, at_y, at_z)

    barrier = pltpu.get_barrier_semaphore()
    peers = [partner] + [ax(d) for ax in axes for d in (1, 2, 3)]
    for peer in peers:
        pl.semaphore_signal(barrier, inc=1, device_id=peer, device_id_type=MESH)

    def mixed_copy(t):
        s = t // 2
        dx, dy = coords(s)
        column = ((((x + dx) % 4) * 4 + (y + dy) % 4) * 2 + (zl + t) % 2) * 128
        return pltpu.make_async_copy(
            mixed_hbm.at[:, pl.ds(pl.multiple_of(column, 128), 128)], mbuf.at[t], msem.at[t]
        )

    counts_copy = pltpu.make_async_copy(counts_hbm, counts_v, in_sem.at[0])
    base_copy = pltpu.make_async_copy(base_hbm, base_v, in_sem.at[1])
    other_copy = pltpu.make_async_copy(other_hbm, other_v, in_sem.at[2])
    base_copy.start()
    other_copy.start()
    counts_copy.start()
    for t in range(AHEAD):
        mixed_copy(t).start()

    lane = lax.broadcasted_iota(jnp.int32, (32, 128), 1)
    row = lax.broadcasted_iota(jnp.int32, (32, 128), 0)
    repeat = (lane % 32 == row).astype(jnp.float32).astype(jnp.bfloat16)
    base_copy.wait()
    other_copy.wait()
    for r in range(0, 2048, 256):
        rs = pl.ds(r, 256)
        for wide, runs in ((a4, base_v), (b4, other_v)):
            wide[rs, :] = lax.dot_general(
                runs[:, rs], repeat, (((0,), (0,)), ((), ())), preferred_element_type=jnp.float32
            )
    counts_copy.wait()
    for r in range(0, 256, 16):
        rs = pl.ds(r, 16)
        cbf[rs, :] = counts_v[rs, :].astype(jnp.float32).astype(jnp.bfloat16)

    lane256 = lax.broadcasted_iota(jnp.int32, (DEPTH, 128), 1)

    def moments_of(rs):
        av, bv = a4[rs, :], b4[rs, :]
        tail = jnp.where(lane256 == 64, 1.0, 0.0)
        value = jnp.where(lane256 < 32, av + bv, jnp.where(lane256 < 64, av * av + bv * bv, tail))
        return value.astype(jnp.bfloat16)

    def terms_of(t, rs):
        change = mbuf[t, rs, :].astype(jnp.float32) - a4[rs, :]
        cross = (b4[rs, :] * change).astype(jnp.bfloat16)
        square = (change * change).astype(jnp.bfloat16)
        return jnp.concatenate([cross, square], axis=1)

    def resampled(make):
        total = None
        for r in range(0, 2048, DEPTH):
            piece = jnp.dot(
                cbf[:, r : r + DEPTH], make(pl.ds(r, DEPTH)), preferred_element_type=jnp.float32
            )
            total = piece if total is None else total + piece
        return total

    sums = resampled(moments_of)
    for q in range(2):
        for c in range(2):
            ustage[c, q] = sums[q * 128 + c * 64 : q * 128 + c * 64 + 64, :]


    def remote(src, dst, send, recv, target):
        return pltpu.make_async_remote_copy(
            src_ref=src, dst_ref=dst, send_sem=send, recv_sem=recv,
            device_id=target, device_id_type=MESH,
        )

    def u_d2d():
        return remote(ustage.at[1 - core], upart, usend.at[0], urecv.at[0], partner)

    def u_z(d):
        target_zh = ((z + d) % 4) // 2
        return remote(upart.at[target_zh], uz.at[d - 1], usend.at[d], urecv.at[d], at_z(d))

    def u_y(d):
        return remote(uz.at[3], uy.at[d - 1], usend.at[3 + d], urecv.at[3 + d], at_y(d))

    def u_x(d):
        return remote(uy.at[3], ux.at[d - 1], usend.at[6 + d], urecv.at[6 + d], at_x(d))

    def u_fin():
        return remote(ux.at[3], ufin.at[core], usend.at[10], urecv.at[10], partner)


    def u_stage1():
        u_d2d().wait_recv()
        for q in range(2):
            upart[q] = upart[q] + ustage[core, q]
        for d in (1, 2, 3):
            u_z(d).start()

    def u_stage2():
        for d in (1, 2, 3):
            u_z(d).wait_recv()
        uz[3] = upart[zh] + uz[0] + uz[1] + uz[2]
        for d in (1, 2, 3):
            u_y(d).start()

    def u_stage3():
        for d in (1, 2, 3):
            u_y(d).wait_recv()
        uy[3] = uz[3] + uy[0] + uy[1] + uy[2]
        for d in (1, 2, 3):
            u_x(d).start()

    def u_stage4():
        for d in (1, 2, 3):
            u_x(d).wait_recv()
        ux[3] = uy[3] + ux[0] + ux[1] + ux[2]
        u_fin().start()

    lane128 = lax.broadcasted_iota(jnp.int32, (128, 128), 1)

    def d2d(t):
        dx, dy = ORDER[t // 2]
        return remote(
            stage.at[t, 1 - core], part.at[dx, dy, t % 2], d2d_send, d2d_recv.at[t], partner
        )

    def multiply(t, dzl):
        result = resampled(lambda rs: terms_of(t, rs))
        carry = (zl + dzl) // 2
        for q in range(2):
            cross = result[q * 128 : q * 128 + 128, :128]
            square = result[q * 128 : q * 128 + 128, 128:]
            j = (q + zh + carry) % 2
            stage[t, 0, j] = jnp.where(lane128 < 64, cross, pltpu.roll(square, 64, 1))
            stage[t, 1, j] = jnp.where(lane128 < 64, pltpu.roll(cross, 64, 1), square)

    def compute(s):
        t = 2 * s

        @pl.when(t + AHEAD < 2 * STEPS)
        def _():
            mixed_copy(t + AHEAD).start()
            mixed_copy(t + AHEAD + 1).start()

        mixed_copy(t).wait()
        mixed_copy(t + 1).wait()
        multiply(t, 0)
        multiply(t + 1, 1)

    def view(color, phase, d, other, h):
        if phase == 1:
            where = ((d, *other), (*other, d), (*other, d % 2, d // 2))[color]
        elif phase == 2:
            where = ((0, d), (*other, 0, d % 2, d // 2), (d, *other, 0, 0))[color]
        else:
            where = ((0, 0, d % 2, d // 2), (d, 0, 0, 0), (0, d, 0, 0))[color]
        first, count = ROWS[color][h]
        if len(bufs[phase][color]) == 1:
            count += ROWS[color][1][1]
        full = (slice(None),) * (4 - len(where))
        return part.at[(*where, *full, pl.ds(first, count))]

    def message(color, phase, d, other, h, direction):
        flat = sum(o * 4**i for i, o in enumerate(other))
        if phase == 1:
            sem = recv_c.at[h, d - 1, flat] if color == 2 else recv1.at[color, h, d - 1, flat]
        elif phase == 2:
            sem = recv2.at[color, d - 1, flat]
        else:
            sem = recv3.at[color, d - 1]
        return remote(
            view(color, phase, d, other, h), bufs[phase][color][h].at[(d - 1, *other)],
            send.at[phase - 1, color, h], sem, axes[(color + phase - 1) % 3](direction),
        )

    def launch(color, phase, d, other):
        if d != 3:
            h = 1 if d == 1 else 0
            message(color, phase, d, other, h, 1).start()
        if d != 1:
            h = 0 if d == 3 else 1
            message(color, phase, d, other, h, 3).start()

    def forward(color, phase, d, other):
        h = 0 if d == 1 else 1
        message(color, phase, 2, other, h, d).wait_recv()
        here = view(color, phase, d, other, h)
        here[...] = here[...] + bufs[phase][color][h][(1, *other)]
        message(color, phase, d, other, h, d).start()

    def arrive(color, phase, other):
        for h in range(2):
            for d in (1, 3):
                message(color, phase, d, other, h, d).wait_recv()
            buf = bufs[phase][color][h]
            here = view(color, phase, 0, other, h)
            here[...] = here[...] + buf[(0, *other)] + buf[(2, *other)]

    def direct(color, phase, d, other):
        for h in range(len(bufs[phase][color])):
            message(color, phase, d, other, h, d).start()

    def gather(color, phase, other):
        for h, buf in enumerate(bufs[phase][color]):
            for d in (1, 2, 3):
                message(color, phase, d, other, h, d).wait_recv()
            here = view(color, phase, 0, other, h)
            here[...] = (here[...] + buf[(0, *other)]) + (buf[(1, *other)] + buf[(2, *other)])

    def exchange(i):
        d2d(2 * i).start()
        d2d(2 * i + 1).start()

    def combine(i):
        dx, dy = ORDER[i]
        for dzl in range(2):
            d2d(2 * i + dzl).wait_recv()
            for j in range(2):
                part[dx, dy, dzl, j] = part[dx, dy, dzl, j] + stage[2 * i + dzl, core, j]
        leave = [direct if color in DIRECT else launch for color in range(3)]
        if dx:
            leave[0](0, 1, dx, (dy,))
        if dy:
            leave[1](1, 1, dy, (dx,))
        for dz in (2, 1, 3):
            leave[2](2, 1, dz, (dx, dy))

    def enter():
        pl.semaphore_wait(barrier, len(peers))
        u_d2d().start()

    work, last = order_of_work()
    does = dict(exchange=exchange, combine=combine, launch=launch, forward=forward, arrive=arrive, direct=direct, gather=gather)
    todo = [(time, count, functools.partial(does[name], *args)) for time, count, name, args in work]
    todo.append((ENTER, -1, enter))
    for i, u_stage in enumerate((u_stage1, u_stage2, u_stage3, u_stage4)):
        todo.append((ENTER + 2 + 5 * i, -1, u_stage))
    todo.sort(key=lambda item: item[:2])
    final = [item for item in todo if item[0] >= min(last)]
    todo = todo[: len(todo) - len(final)]

    @pl.loop(0, STEPS)
    def _(s):
        compute(s)
        for quarter in range(0, STEPS, 4):

            @pl.when(s // 4 == quarter // 4)
            def _(quarter=quarter):
                for step in range(quarter, quarter + 4):
                    now = [run for time, count, run in todo if step - 1 < time <= step]
                    if now:

                        @pl.when(s == step)
                        def _(now=now):
                            for run in now:
                                run()

    for time, count, run in todo:
        if time > STEPS - 1:
            run()

    u_fin().wait_recv()
    ufin[core] = ux[3]
    rolled = []
    for c in range(2):
        sums_c = ufin[c]
        weight = jnp.maximum(sums_c[:, 64:65], 1.0)
        mean = sums_c / (2.0 * weight)
        square_mean = pltpu.roll(sums_c, 96, 1) / (2.0 * weight)
        variance = jnp.maximum(square_mean - mean * mean, 0.25)
        lanes = lax.broadcasted_iota(jnp.int32, (64, 128), 1)
        scaled = jnp.where(lanes < 32, weight * variance, 0.0)
        scaled = scaled + pltpu.roll(scaled, 32, 1)
        scaled = scaled + pltpu.roll(scaled, 64, 1)
        rolled.append(jnp.where(lanes < 64, scaled, 2.0 * scaled))
    divisor = jnp.concatenate(rolled, axis=0)

    def all_left(ref, sem):
        pltpu.make_async_copy(ref, ref, sem).wait()

    all_left(stage.at[:, 0], d2d_send)
    u_d2d().wait_send()
    for d in (1, 2, 3):
        u_z(d).wait_send()
        u_y(d).wait_send()
        u_x(d).wait_send()
    u_fin().wait_send()

    for phase, colors in bufs.items():
        if phase == 3:
            divisor_ref[...] = divisor.T
            for time, count, run in final:
                run()
            sums_ref[...] = part[0, 0, 0, 0].T
        for color in range(3):
            for h, buf in enumerate(colors[color]):
                all_left(buf, send.at[phase - 1, color, h])


def shards(base_runs, other_runs, mixed_runs, counts):
    f32, bf16 = jnp.float32, jnp.bfloat16
    dma = pltpu.SemaphoreType.DMA

    def vmem(*shape, dtype=f32):
        return pltpu.VMEM(shape, dtype)

    sizes = [[count for first, count in color] for color in ROWS]
    scratch = [
        vmem(32, 2048, dtype=bf16), vmem(32, 2048, dtype=bf16), vmem(256, 2048, dtype=jnp.int32),
        vmem(256, 2048, dtype=bf16), vmem(2048, 128), vmem(2048, 128),
        vmem(32, 2048, 128, dtype=bf16),
        vmem(32, 2, 2, 128, 128), vmem(4, 4, 2, 2, 128, 128),
    ]
    inside = (
        ((3, 4, 2, 2), (3, 4, 2, 2), (3, 4, 4)),
        ((3, 2, 2), (3, 4), (3, 4)),
        ((3,), (3,), (3,)),
    )
    scratch.append({
        phase: [
            [
                vmem(*shapes[color], count, 128)
                for count in ([sum(sizes[color])] if phase > 1 or color in DIRECT else sizes[color])
            ]
            for color in range(3)
        ]
        for phase, shapes in enumerate(inside, 1)
    })
    scratch += [
        vmem(2, 2, 64, 128), vmem(2, 64, 128), vmem(4, 64, 128), vmem(4, 64, 128),
        vmem(4, 64, 128), vmem(2, 64, 128),
        dma((3,)), dma((32,)), dma, dma((32,)),
        dma((2, 2, 3, 4)), dma((2, 3, 16)), dma((3, 3, 4)), dma((3, 3)), dma((3, 3, 2)),
        dma((11,)), dma((11,)),
    ]
    any_spec = pl.BlockSpec(memory_space=pl.ANY)
    out = jax.ShapeDtypeStruct((128, 128), f32)
    sums, divisor = pl.pallas_call(
        kernel,
        out_shape=(out, out),
        in_specs=[any_spec] * 4,
        out_specs=(pl.BlockSpec(memory_space=pltpu.VMEM),) * 2,
        scratch_shapes=scratch,
        compiler_params=pltpu.CompilerParams(
            collective_id=0, has_side_effects=True, vmem_limit_bytes=64 * 1024 * 1024 - 65536
        ),
    )(base_runs.T, other_runs.T, mixed_runs, counts)
    return (sums[:64] / divisor[:64]).T, (sums[64:] / divisor[64:]).T


def solution(mesh):
    split = Mesh(mesh.devices.reshape(4, 4, 2, 2, mesh.shape["res"]), AXES)
    every = AXES
    columns = ("x", "y", "zl", "core")
    placed = (P(every, None), P(every, None), P(every, None), P(None, every))
    return jax.shard_map(
        shards,
        mesh=split,
        in_specs=placed,
        out_specs=(P("zh", columns), P("zh", columns)),
        check_vma=False,
    )
```
